256 devices in a mesh: seq: 32 (over y, z), exp: 8 (over x, core).
Axes of the slice: x: 4, y: 4, z: 8, core: 2. Of those that a mesh axis runs over, the one named last changes fastest.
Arguments:
- projected: bfloat16 [3, 4096, 4096], P(None, 'seq', 'exp'), may hold values from -6 to 6
- stream: bfloat16 [4096, 4096], P('seq', 'exp'), may hold values from -6 to 6
- short_filter: float32 [3, 3, 4096], P(None, None, 'exp'), may hold values from -3.5 to 3.5
- long_filter: float32 [4096, 4096], P('seq', 'exp'), may hold values from -0.09375 to 0.09375
- skip_gain: float32 [4096], P('exp'), may hold values from 0.25 to 1.75
- norm_gain: float32 [4096], P('exp'), may hold values from 0.25 to 1.75
- gate_up: bfloat16 [64, 4096, 2, 1408], P('seq', 'exp'), may hold values from -0.125 to 0.125
- down_weight: bfloat16 [64, 1408, 4096], P('seq', None, 'exp'), may hold values from -0.15625 to 0.15625
- expert_ids: int32 [4096, 6], P('seq'), may hold values from 0 to 63, all different within a row; in each aligned block of 128 rows (0 to 127, 128 to 255, ...) at most 16 rows name the same one
- gate_weights: float32 [4096, 6], P('seq'), may hold values from 0.2 to 1
Outputs:
- mixed: bfloat16 [4096, 4096], P('seq', 'exp')
The draws below stay inside these ranges and needn't reach their ends.
Inputs may be any that keep to these rules, and one draw needn't show every extreme that they name: `expert_ids`: each row names 6 different experts. In each aligned block of 128 rows (the rows of one index of seq) no expert is named more than 16 times, a bound that some block reaches.
All inputs are finite; a program needn't handle non-finite values.
Results may differ from the reference program's by a relative error of at most 0.022.
Values may be sent and summed in bfloat16 or wider, within the bound.
A program may use at most 192 MiB of HBM per device.

```python
import math
import jax
import jax.numpy as jnp
import numpy as np
from jax import lax

D = 4096
FF = 1408
TOP = 6
TAPS = 3
TOK_DEV = 128
LENGTH = 4096
EXPERTS = 64
CAP = 16
N_SEQ = 32
N_EXP = 8


def with_spikes(values, own_key, source, target, parts, factor):
    owner, partner = [(jnp.arange(values.shape[axis_at]) // (values.shape[axis_at] // parts)).reshape([-1 if axis == axis_at else 1 for axis in range(values.ndim)]) for axis_at in (source, target)]
    chosen = jax.random.permutation(own_key, parts)[partner]
    strong = (owner == chosen) | (owner == (partner + parts // 2) % parts)
    return jnp.where(strong, factor * values, values)


def steps_of(key, dims, shards, least, largest):
    level = 1.0
    for dim, blocks in shards:
        draws = jax.random.uniform(jax.random.fold_in(jax.random.fold_in(key, 6), dim), (blocks,), jnp.float32, least / len(shards), largest / len(shards))
        level = level * jnp.repeat(jnp.exp(draws), dims[dim] // blocks).reshape((-1,) + (1,) * (len(dims) - 1 - dim))
    return level


def routed_block(key, own, number, rows, count, top, limit, slope):
    ranking = jax.random.permutation(key, count)
    heavy_load, common = portions_of(count, rows * top, limit, slope, True), portions_of(count, rows * top, limit, slope, False)
    places = jnp.arange(count)

    def named(sizes, turn):
        used = int((sizes > 0).sum())
        fixed = max(1, used // 4)
        moved = fixed + (places - fixed + turn * (used - fixed)) % max(1, count - fixed)
        return jnp.zeros((count,), jnp.int32).at[ranking[jnp.where(places < fixed, places, moved)]].set(jnp.asarray(sizes, jnp.int32))

    sizes = jnp.where(number % 4 == 0, named(heavy_load, number // 4), named(common, number - number // 4 - 1))
    mixed = jax.random.permutation(jax.random.fold_in(own, 3), count)
    donor, receiver = mixed[0:count // 2 * 2:2], mixed[1:count // 2 * 2:2]
    room = jnp.minimum(sizes[donor] - 1, limit - sizes[receiver]) // 2
    room = jnp.where((donor == ranking[0]) | (receiver == ranking[0]) | (sizes[receiver] == 0), 0, jnp.maximum(room, 0))
    moved = jax.random.randint(jax.random.fold_in(own, 4), (count // 2,), 0, 1 << 20) % (room + 1)
    sizes = sizes.at[donor].add(-moved).at[receiver].add(moved)
    items = jnp.searchsorted(jnp.cumsum(sizes), jnp.arange(rows * top), side="right").astype(jnp.int32)
    grid = items.reshape(top, rows).T
    grid = grid[jax.random.permutation(jax.random.fold_in(own, 1), rows)]
    turn = jax.random.randint(jax.random.fold_in(own, 2), (rows, 1), 0, top)
    return jnp.take_along_axis(grid, (jnp.arange(top)[None, :] + turn) % top, axis=1)


def portions_of(number_of, total, reach, skew, full):
    portions = [(1 << 20) // math.isqrt(grade ** skew) + 1 for grade in range(1, number_of + 1)]
    largest = reach if full else min(reach, max(-(-total // number_of), total * portions[0] // sum(portions)))
    least = 1 if total - largest >= number_of - 1 else 0
    holding, spare = [largest] + [least] * (number_of - 1), total - largest - least * (number_of - 1)
    while spare > 0:
        candidates = [i for i in range(1, number_of) if holding[i] < largest] or [i for i in range(1, number_of) if holding[i] < reach]
        mass, left = sum([portions[i] for i in candidates]), spare
        for i in candidates:
            addition = min(reach - holding[i], max(1, left * portions[i] // mass), spare)
            holding[i] = holding[i] + addition
            spare = spare - addition
    return np.array(holding)


def gaussian(rng, extent, width, reach, shards=(), held_as=jnp.bfloat16):
    array = jax.random.normal(rng, extent, jnp.float32) * width
    if len(shards) > 0:
        array = steps_of(rng, extent, shards, -0.22, 0.18) * array
    return jnp.clip(array, min=-reach, max=reach).astype(held_as)


def gaussian_with(own_key, extent, width, limit, pieces, heavy, held_as=jnp.bfloat16):
    result = width * jax.random.normal(own_key, extent, jnp.float32)
    if pieces:
        result = result * steps_of(own_key, extent, pieces, -0.22, 0.18)
    return jnp.clip(with_spikes(result, jax.random.fold_in(own_key, 3), *heavy), -limit, limit).astype(held_as)


def setup_inputs(seed: int = 0) -> dict:
    key_of = jax.random.split(jax.random.key(seed), 11)
    projected = gaussian(key_of[0], (3, LENGTH, D), 1.0, 6.0, ((1, 32), (2, 8)))
    stream = gaussian(key_of[1], (LENGTH, D), 1.0, 6.0, ((0, 32), (1, 8)))
    short_filter = gaussian(key_of[2], (3, TAPS, D), TAPS ** -0.5, 3.5, ((2, 8),), jnp.float32)
    long_filter = gaussian(key_of[3], (LENGTH, D), LENGTH ** -0.5, 0.09375, ((0, 32), (1, 8)), jnp.float32)
    skip_gain = jnp.clip(1.0 + 0.15 * jax.random.normal(key_of[4], (D,), jnp.float32), 0.25, 1.75)
    norm_gain = jnp.clip(1.0 + 0.15 * jax.random.normal(key_of[5], (D,), jnp.float32), 0.25, 1.75)
    gate_up = gaussian_with(key_of[6], (EXPERTS, D, 2, FF), D ** -0.5, 0.125, ((0, 32), (1, 8)), (1, 3, 8, 2.0))
    down_weight = gaussian(key_of[7], (EXPERTS, FF, D), FF ** -0.5, 0.15625, ((0, 32), (2, 8)))
    expert_ids_keys = jax.random.split(jax.random.fold_in(key_of[8], 1), LENGTH // TOK_DEV)
    expert_ids_turns = jax.random.permutation(jax.random.fold_in(key_of[8], 3), LENGTH // TOK_DEV)
    expert_ids = jax.vmap(lambda own, number: routed_block(jax.random.fold_in(key_of[8], 2), own, number, TOK_DEV, EXPERTS, TOP, CAP, 2))(expert_ids_keys, expert_ids_turns).reshape((LENGTH, TOP))
    gate_weights = jnp.clip(0.2 + 0.8 * jax.random.uniform(key_of[9], (LENGTH, TOP), jnp.float32) ** steps_of(key_of[9], (LENGTH, TOP), ((0, 32),), -0.2, 0.2), 0.2, 1.0)
    return {"projected": projected, "stream": stream, "short_filter": short_filter, "long_filter": long_filter, "skip_gain": skip_gain, "norm_gain": norm_gain, "gate_up": gate_up, "down_weight": down_weight, "expert_ids": expert_ids, "gate_weights": gate_weights}


def reference(projected, stream, short_filter, long_filter, skip_gain, norm_gain, gate_up, down_weight, expert_ids, gate_weights):
    values = projected.astype(jnp.float32)
    length = values.shape[1]
    mixed_short = short_filter[:, 0][:, None, :] * values
    for offset in range(1, TAPS):
        shifted = jnp.pad(values, ((0, 0), (offset, 0), (0, 0)))[:, :length]
        mixed_short = mixed_short + short_filter[:, offset][:, None, :] * shifted
    queries = mixed_short[0]
    key_side = mixed_short[1]
    valued = mixed_short[2]
    product = key_side * valued
    spectrum = jnp.fft.rfft(product, n=2 * length, axis=0) * jnp.fft.rfft(long_filter, n=2 * length, axis=0)
    convolved = jnp.fft.irfft(spectrum, n=2 * length, axis=0)[:length]
    mixed_long = queries * (convolved + skip_gain * product)
    residual = (stream.astype(jnp.float32) + mixed_long).astype(jnp.bfloat16)
    resid_float = residual.astype(jnp.float32)
    root_mean = jnp.sqrt(lax.optimization_barrier(jnp.sum(resid_float * resid_float, axis=1)) / D + 1e-06)
    normed = (resid_float / root_mean[:, None] * norm_gain).astype(jnp.bfloat16)
    block_ids_flat = expert_ids.reshape(N_SEQ, TOK_DEV * TOP)
    onehot = (block_ids_flat[:, :, None] == jnp.arange(EXPERTS, dtype=jnp.int32)[None, None, :]).astype(jnp.int32)
    slot_ids = lax.optimization_barrier(jnp.sum((jnp.cumsum(onehot, axis=1) - onehot) * onehot, axis=2)).astype(jnp.int32)
    block_ids = jnp.broadcast_to(jnp.arange(N_SEQ, dtype=jnp.int32)[:, None], block_ids_flat.shape)
    token_ids = block_ids * TOK_DEV + jnp.arange(TOK_DEV * TOP, dtype=jnp.int32)[None, :] // TOP
    slot_table = jnp.zeros((EXPERTS, N_SEQ, CAP), jnp.int32).at[block_ids_flat, block_ids, slot_ids].set(token_ids + 1)
    padded = jnp.concatenate([jnp.zeros((1, D), jnp.bfloat16), normed], axis=0)

    def one_expert(running, input_rows):
        sources, weights_in, output_weight = input_rows
        gathered = padded[sources.reshape(-1)].astype(jnp.float32).reshape(-1, N_EXP, D // N_EXP)
        blocked = weights_in.astype(jnp.float32).reshape(N_EXP, D // N_EXP, 2 * FF)
        partials = jnp.einsum('rbc,bcf->rbf', gathered, blocked)
        rounded = lax.optimization_barrier(partials.astype(jnp.bfloat16))
        totals = lax.optimization_barrier(jnp.sum(rounded.astype(jnp.float32), axis=1))
        hidden_state = (jax.nn.silu(totals[:, :FF]) * totals[:, FF:]).astype(jnp.bfloat16)
        final_output = jnp.dot(hidden_state, output_weight, preferred_element_type=jnp.float32).astype(jnp.bfloat16)
        return (running, final_output)
    unused, expert_out = lax.scan(one_expert, jnp.zeros((), jnp.float32), (slot_table, gate_up, down_weight))
    flat_out = expert_out.reshape(EXPERTS * N_SEQ * CAP, D)
    position = (block_ids_flat * (N_SEQ * CAP) + block_ids * CAP + slot_ids).reshape(N_SEQ * TOK_DEV, TOP)
    combined = jnp.zeros((length, D), jnp.float32)
    for pick_k in range(TOP):
        combined = combined + gate_weights[:, pick_k:pick_k + 1] * flat_out[position[:, pick_k]].astype(jnp.float32)
    return (resid_float + combined).astype(jnp.bfloat16)
```

```python
import math

import jax
import jax.numpy as jnp
from jax import lax
from jax.experimental import pallas as pl
from jax.experimental.pallas import tpu as pltpu
from jax.sharding import PartitionSpec as P

D = 4096


def shifted(value, axis, by):
    devices = lax.axis_size(axis)
    pairs = [(i, i + by) for i in range(devices) if 0 <= i + by < devices]
    return lax.ppermute(value, axis, pairs)


def copy_for_each(value, axis):
    copies = jnp.broadcast_to(value, (lax.axis_size(axis), *value.shape))
    return lax.all_to_all(copies, axis, split_axis=0, concat_axis=0, tiled=True)


def over_copies(value, axis):
    everything = copy_for_each(value, axis)
    return jnp.sum(everything, axis=0)


def angle_table(left_ids, right_ids, modulus):
    product = left_ids[:, None] * right_ids[None, :] % modulus
    return 2.0 * math.pi / modulus * product.astype(jnp.float32)


def precise(formula, matrix, operand):
    return jnp.einsum(formula, matrix, operand, precision=lax.Precision.HIGHEST)


def local_long(whole, slab_count, tok_rows):
    blocks = 2 * slab_count
    points = blocks * tok_rows
    width = whole.shape[2]
    arranged = whole.reshape(2, slab_count, tok_rows, width)
    slab_ids = jnp.arange(slab_count, dtype=jnp.int32)
    frequency_index = jnp.arange(blocks, dtype=jnp.int32)
    row_ids = jnp.arange(tok_rows, dtype=jnp.int32)
    outer_angle = angle_table(frequency_index, slab_ids, blocks)
    first_re = precise("kp,apmc->akmc", jnp.cos(outer_angle), arranged)
    first_im = -precise("kp,apmc->akmc", jnp.sin(outer_angle), arranged)
    twiddle = angle_table(frequency_index, row_ids, points)
    turn_cos = jnp.cos(twiddle)[None, :, :, None]
    turn_sin = jnp.sin(twiddle)[None, :, :, None]
    turned_re = first_re * turn_cos + first_im * turn_sin
    turned_im = first_im * turn_cos - first_re * turn_sin
    inner_rotation = angle_table(row_ids, row_ids, tok_rows)
    inner_cos = jnp.cos(inner_rotation)
    inner_sin = jnp.sin(inner_rotation)
    spec_re = precise("qm,akmc->akqc", inner_cos, turned_re) + precise(
        "qm,akmc->akqc", inner_sin, turned_im
    )
    spec_im = precise("qm,akmc->akqc", inner_cos, turned_im) - precise(
        "qm,akmc->akqc", inner_sin, turned_re
    )
    joint_re = spec_re[0] * spec_re[1] - spec_im[0] * spec_im[1]
    joint_im = spec_re[0] * spec_im[1] + spec_im[0] * spec_re[1]
    back_re = precise("mq,kqc->kmc", inner_cos, joint_re) - precise(
        "mq,kqc->kmc", inner_sin, joint_im
    )
    back_im = precise("mq,kqc->kmc", inner_cos, joint_im) + precise(
        "mq,kqc->kmc", inner_sin, joint_re
    )
    back_cos = jnp.cos(twiddle)[:, :, None]
    back_sin = jnp.sin(twiddle)[:, :, None]
    reverted_re = back_re * back_cos - back_im * back_sin
    reverted_im = back_re * back_sin + back_im * back_cos
    last_angle = angle_table(slab_ids, frequency_index, blocks)
    inverted = (
        precise("pk,kmc->pmc", jnp.cos(last_angle), reverted_re)
        - precise("pk,kmc->pmc", jnp.sin(last_angle), reverted_im)
    ) / points
    return inverted.reshape(slab_count * tok_rows, width)


MESH = pl.DeviceIdType.MESH
SLOTS = 16
HALF = 512
HIDDEN = 1408


def dot(left, right):
    return jnp.dot(left, right, preferred_element_type=jnp.float32)


def remote(src, dst, send, recv, seq, exp):
    return pltpu.make_async_remote_copy(
        src_ref=src,
        dst_ref=dst,
        send_sem=send,
        recv_sem=recv,
        device_id=(seq, exp),
        device_id_type=MESH,
    )


def rows(start, size):
    return pl.ds(pl.multiple_of(start, size), size)


def experts_kernel(
    normed,
    resid,
    ids,
    weights,
    gate_up,
    down,
    out,
    packed,
    recv,
    wg,
    wd,
    far_out,
    far_in,
    near_out,
    near_in,
    held,
    hidden,
    outgoing,
    returned,
    chosen_hi,
    chosen_lo,
    local_sem,
    swap_send,
    swap_recv,
    out_send,
    out_recv,
    far_send,
    far_recv,
    near_send,
    near_recv,
    hid_send,
    hid_recv,
    fwd_send,
    fwd_recv,
    back_send,
    back_recv,
):
    seq = lax.axis_index("seq")
    exp = lax.axis_index("exp")
    core = lax.rem(exp, 2)
    chip = exp // 2
    column = 2 * chip
    partner = column + 1 - core
    after = lax.rem(chip + 1, 4)
    before = lax.rem(chip + 3, 4)
    across = lax.rem(chip + 2, 4)
    exp_after = 2 * after + core
    exp_before = 2 * before + core

    own_gate = pltpu.make_async_copy(gate_up.at[core], wg.at[core], local_sem.at[0])
    own_down = pltpu.make_async_copy(down.at[core], wd.at[core], local_sem.at[1])
    own_gate.start()
    own_down.start()

    barrier = pltpu.get_barrier_semaphore()

    def greet(i, carry):
        other = lax.rem(seq + i, 32)
        for side in range(2):
            pl.semaphore_signal(barrier, inc=1, device_id=(other, column + side), device_id_type=MESH)
        return carry

    lax.fori_loop(1, 32, greet, 0)
    for other in (partner, exp_after, exp_before):
        pl.semaphore_signal(barrier, inc=1, device_id=(seq, other), device_id_type=MESH)

    tokens = ids.shape[0]
    lanes = lax.broadcasted_iota(jnp.int32, (tokens, 128), 1)
    named = jnp.zeros((tokens, 128), jnp.float32)
    scale = jnp.zeros((tokens, 128), jnp.float32)
    for k in range(ids.shape[1]):
        hit = ids[:, k : k + 1] == lanes
        named = jnp.where(hit, 1.0, named)
        scale = jnp.where(hit, weights[:, k : k + 1], scale)
    row_ids = lax.broadcasted_iota(jnp.int32, (tokens, tokens), 0)
    col_ids = lax.broadcasted_iota(jnp.int32, (tokens, tokens), 1)
    earlier = jnp.where(col_ids < row_ids, 1.0, 0.0).astype(jnp.bfloat16)
    rank = dot(earlier, named.astype(jnp.bfloat16))
    number = named * (rank + 1.0)
    slot_rows = 64 * SLOTS
    spread_row = lax.broadcasted_iota(jnp.int32, (slot_rows, 128), 0)
    spread_col = lax.broadcasted_iota(jnp.int32, (slot_rows, 128), 1)
    spread = jnp.where(spread_row // SLOTS == spread_col, 1.0, 0.0).astype(jnp.bfloat16)
    number_rows = dot(spread, number.T.astype(jnp.bfloat16))
    wanted = (lax.rem(spread_row, SLOTS) + 1).astype(jnp.float32)
    pick = jnp.where(number_rows == wanted, 1.0, 0.0).astype(jnp.bfloat16)
    packed[...] = dot(pick, normed[...]).astype(jnp.bfloat16)

    own_row = (core * 32 + seq) * SLOTS
    pl.semaphore_wait(barrier, 65)

    swap_gate = remote(gate_up.at[1 - core], wg.at[core], swap_send.at[0], swap_recv.at[0], seq, partner)
    swap_down = remote(down.at[1 - core], wd.at[core], swap_send.at[1], swap_recv.at[1], seq, partner)
    swap_gate.start()

    def send_rows(other, side):
        remote(
            packed.at[rows((2 * other + side) * SLOTS, SLOTS)],
            recv.at[rows(own_row, SLOTS)],
            out_send,
            out_recv,
            other,
            column + side,
        ).start()

    def dispatch(i, carry):
        other = lax.rem(seq + i, 32)
        for side in range(2):
            send_rows(other, side)
        return carry

    lax.fori_loop(1, 32, dispatch, 0)
    send_rows(seq, 1 - core)
    swap_down.start()
    recv[rows(own_row, SLOTS)] = packed[rows((2 * seq + core) * SLOTS, SLOTS)]

    turn_row = lax.broadcasted_iota(jnp.int32, (128, slot_rows), 0)
    turn_col = lax.broadcasted_iota(jnp.int32, (128, slot_rows), 1)
    turned = jnp.where(turn_col // SLOTS == turn_row, 1.0, 0.0).astype(jnp.bfloat16)
    number_cols = dot(number.astype(jnp.bfloat16), turned)
    matched = number_cols == (lax.rem(turn_col, SLOTS) + 1).astype(jnp.float32)
    scale_hi = scale.astype(jnp.bfloat16)
    scale_lo = (scale - scale_hi.astype(jnp.float32)).astype(jnp.bfloat16)
    chosen_hi[...] = jnp.where(matched, dot(scale_hi, turned), 0.0).astype(jnp.bfloat16)
    chosen_lo[...] = jnp.where(matched, dot(scale_lo, turned), 0.0).astype(jnp.bfloat16)

    own_gate.wait()
    swap_gate.wait()
    received = pl.ds(0, 63 * SLOTS)
    remote(packed.at[received], recv.at[received], out_send, out_recv, seq, partner).wait()

    def partial(quarter, which):
        first = recv[rows(quarter * 128, 128)]
        second = recv[rows(HALF + quarter * 128, 128)]
        return dot(first, wg[0, which]) + dot(second, wg[1, which])

    far_gate = remote(far_out.at[0], far_in.at[0], far_send.at[0], far_recv.at[0], seq, exp_after)
    far_up = remote(far_out.at[1], far_in.at[1], far_send.at[1], far_recv.at[1], seq, exp_before)
    far_out[0] = partial(across, 0).astype(jnp.bfloat16)
    far_gate.start()
    far_out[1] = partial(across, 1).astype(jnp.bfloat16)
    far_up.start()

    def near(direction, which):
        return remote(
            near_out.at[direction, which],
            near_in.at[direction, which],
            near_send.at[direction, which],
            near_recv.at[direction, which],
            seq,
            (exp_after, exp_before)[direction],
        )

    near_out[0, 1] = partial(after, 1).astype(jnp.bfloat16)
    near(0, 1).start()
    near_out[1, 0] = partial(before, 0).astype(jnp.bfloat16)
    near(1, 0).start()
    held[0] = partial(after, 0)
    held[1] = partial(before, 1)
    far_gate.wait_recv()
    near_out[0, 0] = (held[0] + far_in[0].astype(jnp.float32)).astype(jnp.bfloat16)
    near(0, 0).start()
    far_up.wait_recv()
    near_out[1, 1] = (held[1] + far_in[1].astype(jnp.float32)).astype(jnp.bfloat16)
    near(1, 1).start()
    held[0] = partial(chip, 0)
    held[1] = partial(chip, 1)
    near(0, 1).wait_recv()
    near(1, 0).wait_recv()
    near(0, 0).wait_recv()
    near(1, 1).wait_recv()

    gate = held[0] + near_in[0, 0].astype(jnp.float32) + near_in[1, 0].astype(jnp.float32)
    up = held[1] + near_in[0, 1].astype(jnp.float32) + near_in[1, 1].astype(jnp.float32)
    hidden[chip] = (gate / (1.0 + jnp.exp(-gate)) * up).astype(jnp.bfloat16)

    def share(direction):
        return remote(
            hidden.at[chip],
            hidden.at[chip],
            hid_send.at[direction],
            hid_recv.at[direction],
            seq,
            (exp_after, exp_before)[direction],
        )

    def arrived(direction):
        quarter = (before, after)[direction]
        return remote(
            hidden.at[quarter],
            hidden.at[quarter],
            hid_send.at[direction],
            hid_recv.at[direction],
            seq,
            (exp_after, exp_before)[direction],
        )

    def forward(direction, quarter):
        part = pl.ds(64 * direction, 64)
        return remote(
            hidden.at[quarter, part],
            hidden.at[quarter, part],
            fwd_send.at[direction],
            fwd_recv.at[direction],
            seq,
            (exp_after, exp_before)[direction],
        )

    share(0).start()
    share(1).start()
    own_down.wait()
    swap_down.wait()

    back_row = (2 * seq + core) * SLOTS

    def give_back(quarter):
        values = hidden[quarter]
        for side in range(2):
            outgoing[side, rows(quarter * 128, 128)] = dot(values, wd[side]).astype(jnp.bfloat16)

        def send_back(i, carry):
            other = quarter * 8 + lax.rem(seq + i, 8)
            for side in range(2):

                @pl.when(jnp.logical_or(other != seq, side != core))
                def _():
                    remote(
                        outgoing.at[side, rows(other * SLOTS, SLOTS)],
                        returned.at[rows(back_row, SLOTS)],
                        back_send,
                        back_recv,
                        other,
                        column + side,
                    ).start()

            return carry

        lax.fori_loop(0, 8, send_back, 0)

    give_back(chip)
    arrived(0).wait_recv()
    forward(0, before).start()
    arrived(1).wait_recv()
    forward(1, after).start()
    give_back(before)
    give_back(after)
    forward(0, across).wait_recv()
    forward(1, across).wait_recv()
    give_back(across)
    returned[rows(back_row, SLOTS)] = outgoing[core, rows(seq * SLOTS, SLOTS)]

    far_gate.wait_send()
    far_up.wait_send()
    for direction in range(2):
        for which in range(2):
            near(direction, which).wait_send()
        share(direction).wait_send()
    forward(0, before).wait_send()
    forward(1, after).wait_send()

    remote(packed.at[received], returned.at[received], back_send, back_recv, seq, partner).wait()
    combined = dot(chosen_hi[...], returned[...]) + dot(chosen_lo[...], returned[...])
    out[...] = (resid[...].astype(jnp.float32) + combined).astype(jnp.bfloat16)


def experts(normed, resid, ids, weights, gate_up, down):
    tokens, width = normed.shape
    vmem = pl.BlockSpec(memory_space=pltpu.VMEM)
    anywhere = pl.BlockSpec(memory_space=pl.ANY)
    bf16, f32 = jnp.bfloat16, jnp.float32
    dma = pltpu.SemaphoreType.DMA
    return pl.pallas_call(
        experts_kernel,
        out_shape=jax.ShapeDtypeStruct((tokens, width), bf16),
        in_specs=[vmem, vmem, vmem, vmem, anywhere, anywhere],
        out_specs=vmem,
        scratch_shapes=[
            pltpu.VMEM((64 * SLOTS, width), bf16),
            pltpu.VMEM((64 * SLOTS, width), bf16),
            pltpu.VMEM((2, 2, width, HIDDEN), bf16),
            pltpu.VMEM((2, HIDDEN, width), bf16),
            pltpu.VMEM((2, 128, HIDDEN), bf16),
            pltpu.VMEM((2, 128, HIDDEN), bf16),
            pltpu.VMEM((2, 2, 128, HIDDEN), bf16),
            pltpu.VMEM((2, 2, 128, HIDDEN), bf16),
            pltpu.VMEM((2, 128, HIDDEN), f32),
            pltpu.VMEM((4, 128, HIDDEN), bf16),
            pltpu.VMEM((2, HALF, width), bf16),
            pltpu.VMEM((64 * SLOTS, width), bf16),
            pltpu.VMEM((tokens, 64 * SLOTS), bf16),
            pltpu.VMEM((tokens, 64 * SLOTS), bf16),
            dma((2,)),
            dma((2,)),
            dma((2,)),
            dma,
            dma,
            dma((2,)),
            dma((2,)),
            dma((2, 2)),
            dma((2, 2)),
            dma((2,)),
            dma((2,)),
            dma((2,)),
            dma((2,)),
            dma,
            dma,
        ],
        compiler_params=pltpu.CompilerParams(
            collective_id=0, has_side_effects=True, vmem_limit_bytes=48 * 1024 * 1024
        ),
        name="experts",
    )(normed, resid, ids, weights, gate_up, down)


def local(
    projected,
    stream,
    short_filter,
    long_filter,
    skip_gain,
    norm_gain,
    gate_up,
    down_weight,
    expert_ids,
    gate_weights,
):
    seq_count = lax.axis_size("seq")
    tok_rows = projected.shape[1]
    channels = projected.shape[2]
    tap_count = short_filter.shape[1]
    earlier = shifted(projected[:, tok_rows - (tap_count - 1) :, :], "seq", 1)
    extended = jnp.concatenate([earlier, projected], axis=1).astype(jnp.float32)
    mixed_short = short_filter[:, 0][:, None, :] * extended[:, tap_count - 1 :]
    for offset in range(1, tap_count):
        begin = tap_count - 1 - offset
        mixed_short = (
            mixed_short
            + short_filter[:, offset][:, None, :] * extended[:, begin : begin + tok_rows]
        )
    queries = mixed_short[0]
    key_side = mixed_short[1]
    valued = mixed_short[2]
    product = key_side * valued
    paired = jnp.stack([product, long_filter])
    whole = lax.all_to_all(
        paired.astype(jnp.bfloat16), "seq", split_axis=2, concat_axis=1, tiled=True
    ).astype(paired.dtype)
    result_long = local_long(whole, seq_count, tok_rows)
    convolved = lax.all_to_all(
        result_long.astype(jnp.bfloat16), "seq", split_axis=0, concat_axis=1, tiled=True
    ).astype(result_long.dtype)
    mixed_long = queries * (convolved + skip_gain * product)
    residual = (stream.astype(jnp.float32) + mixed_long).astype(jnp.bfloat16)
    resid_float = residual.astype(jnp.float32)
    squared_values = over_copies(jnp.sum(resid_float * resid_float, axis=1), "exp")
    root_mean = jnp.sqrt(squared_values / D + 1e-06)
    normed = (resid_float / root_mean[:, None] * norm_gain).astype(jnp.bfloat16)
    split = jnp.transpose(gate_up, (0, 2, 1, 3))
    return experts(normed, residual, expert_ids, gate_weights, split, down_weight)


def solution(mesh):
    in_specs = (
        P(None, "seq", "exp"),
        P("seq", "exp"),
        P(None, None, "exp"),
        P("seq", "exp"),
        P("exp"),
        P("exp"),
        P("seq", "exp", None, None),
        P("seq", None, "exp"),
        P("seq", None),
        P("seq", None),
    )
    out_specs = P("seq", "exp")
    return jax.shard_map(local, mesh=mesh, in_specs=in_specs, out_specs=out_specs, check_vma=False)
```
